256 devices in a mesh: groups: 4 (over x, y), tp: 64 (over z, core).
Axes of the slice: x: 2, y: 2, z: 32, core: 2. Of those that a mesh axis runs over, the one named last changes fastest.
The devices are a block of a 4x8x32 slice.
Arguments:
- queries: bfloat16 [8, 4096, 4096], P('groups', 'tp'), parts along dimension 0, may hold values from -162 to 162
- keys: bfloat16 [8, 4096, 2048], P('groups', 'tp'), parts along dimension 0, may hold values from -6 to 6
- values: bfloat16 [8, 4096, 2048], P('groups', 'tp'), parts along dimension 0, may hold values from -6 to 6
- lengths: int32 [8], P('groups'), parts along dimension 0, may hold values from 1024 to 4096
Outputs:
- attended: bfloat16 [8, 4096, 4096], P('groups', 'tp'), parts along dimension 0
The draws below stay inside these ranges and needn't reach their ends.
There are 4 independent parts, one for each index of `groups`. The reference program is written for one: setup_inputs(seed, part) draws one part's arguments, and reference() takes and returns one part's arrays. A program takes and returns all parts, laid end to end along the dimension named above; each array names one. Nothing has to cross between parts.
All inputs are finite; a program needn't handle non-finite values.
Results may differ from the reference program's by a relative error of at most 0.0085.
Values may be sent and summed in bfloat16 or wider, within the bound.
No kernel may reach another device: no remote copies, remote signals or barrier semaphores. Data moves between devices by JAX's collectives and lax.ppermute only.
A program may use at most 64 MiB of HBM per device.

```python
import jax
import jax.numpy as jnp
from jax import lax

HEADS = 32
KVH = 16
HD = 128
SEQS = 2
LEN = 4096


def key_field(key):
    sub = jax.random.fold_in(key, 11)
    field = jnp.clip(jax.random.normal(sub, (SEQS, LEN, KVH * HD), jnp.float32), -6.0, 6.0)
    return field


def draw_keys(key, part):
    return key_field(key).astype(jnp.bfloat16)


def draw_queries(key, part):
    field = key_field(key).reshape(SEQS, LEN, KVH, HD)
    subkeys = jax.random.split(jax.random.fold_in(key, 23), 6)
    shape = (SEQS, LEN, HEADS)
    base = jnp.clip(jax.random.normal(subkeys[0], (SEQS, LEN, HEADS, HD), jnp.float32), -6.0, 6.0)
    share = 0.125
    places = jnp.arange(LEN, dtype=jnp.int32)
    reach = jnp.minimum(places + 1, max(LEN // 4, 1))[None, :, None]
    first = jax.random.randint(subkeys[1], shape, 0, reach)
    offset = jax.random.randint(subkeys[2], shape, 0, jnp.maximum(reach - 1, 1))
    second = (first + 1 + offset) % reach
    lead = jax.random.uniform(subkeys[3], shape, jnp.float32, 100.0, 150.0) * (12.0 / HD)
    ratio = jax.random.uniform(subkeys[4], shape, jnp.float32, 0.65, 0.85)
    chosen = jax.random.uniform(subkeys[5], shape, jnp.float32) < share
    seq_index = jnp.arange(SEQS, dtype=jnp.int32)[:, None, None]
    head_index = (jnp.arange(HEADS, dtype=jnp.int32) // 2)[None, None, :]
    pick_first = field[seq_index, first, head_index]
    pick_second = field[seq_index, second, head_index]
    aligned = lead[..., None] * pick_first + (lead * ratio)[..., None] * pick_second
    result = base + jnp.where(chosen[..., None], aligned, 0.0)
    return result.reshape(SEQS, LEN, HEADS * HD).astype(jnp.bfloat16)


def level_of(own_key, shape, cuts, low, top_value):
    level = 1.0
    for dim, blocks in cuts:
        heights = jax.random.uniform(jax.random.fold_in(jax.random.fold_in(own_key, 6), dim), (blocks,), jnp.float32, low / len(cuts), top_value / len(cuts))
        level = level * jnp.repeat(jnp.exp(heights), shape[dim] // blocks).reshape((-1,) + (1,) * (len(shape) - 1 - dim))
    return level


def normal_values(key, shape, scale, most, pieces=(), kind=jnp.bfloat16):
    values = scale * jax.random.normal(key, shape, jnp.float32)
    if pieces:
        values = values * level_of(key, shape, pieces, -0.22, 0.18)
    return jnp.clip(values, -most, most).astype(kind)


def setup_inputs(seed: int = 0, part: int = 0) -> dict:
    key_of = jax.random.split(jax.random.key(seed), 5)
    part_splits = jax.random.split(jax.random.fold_in(key_of[4], part), 5)
    queries = draw_queries(jax.random.fold_in(jax.random.fold_in(key_of[4], part), 71), part)
    keys = draw_keys(jax.random.fold_in(jax.random.fold_in(key_of[4], part), 71), part)
    values = normal_values(part_splits[2], (SEQS, LEN, KVH * HD), 1.0, 6.0, ((1, 64),))
    lengths = jax.random.randint(part_splits[3], (SEQS,), LEN // 4, LEN + 1).astype(jnp.int32)
    return dict(queries=queries, keys=keys, values=values, lengths=lengths)


query_scale = 144.0 ** -0.5
soft_cap = 50.0


def one_head(operands):
    head_q, head_k, head_v, valid = operands
    score = jnp.dot(head_q.astype(jnp.float32), head_k.astype(jnp.float32).T) * query_scale
    capped = soft_cap * jnp.tanh(score / soft_cap)
    places = jnp.arange(LEN)
    allowed = (places[None, :] <= places[:, None]) & (places[None, :] < valid)
    weight = jnp.where(allowed, jnp.exp(capped), 0.0)
    total = jnp.sum(weight, axis=1)
    rounded = weight.astype(jnp.bfloat16)
    mixed = jnp.dot(rounded.astype(jnp.float32), head_v.astype(jnp.float32)) / total[:, None]
    live = places[:, None] < valid
    return jnp.where(live, mixed, 0.0).astype(jnp.bfloat16)


def reference(queries, keys, values, lengths):
    split_q = queries.reshape(SEQS, LEN, HEADS, HD).transpose(0, 2, 1, 3).reshape(SEQS * HEADS, LEN, HD)
    split_k = jnp.repeat(keys.reshape(SEQS, LEN, KVH, HD).transpose(0, 2, 1, 3), 2, axis=1).reshape(SEQS * HEADS, LEN, HD)
    split_v = jnp.repeat(values.reshape(SEQS, LEN, KVH, HD).transpose(0, 2, 1, 3), 2, axis=1).reshape(SEQS * HEADS, LEN, HD)
    valid = jnp.repeat(lengths.astype(jnp.int32), HEADS)
    result = lax.map(one_head, (split_q, split_k, split_v, valid))
    return result.reshape(SEQS, HEADS, LEN, HD).transpose(0, 2, 1, 3).reshape(SEQS, LEN, HEADS * HD)
```

```python
import functools

import jax
import jax.numpy as jnp
from jax import lax
from jax.experimental import pallas as pl
from jax.experimental.pallas import tpu as pltpu
from jax.sharding import Mesh
from jax.sharding import PartitionSpec as P

HEADS = 32
KVH = 16
HD = 128
SHARED = HEADS // KVH
CORES = 2
RING, CORE = "tp_0", "tp_1"

query_scale = 144.0 ** (-0.5)
soft_cap = 50.0
tanh_scale = query_scale / soft_cap
exp_scale = soft_cap * 1.4426950408889634

TILE_CHUNKS = 4


def vmem():
    return pl.BlockSpec(memory_space=pltpu.VMEM)


def smem():
    return pl.BlockSpec(memory_space=pltpu.SMEM)


def first_rows(count, lanes):
    return pl.BlockSpec((count, lanes), lambda i: (0, 0))


def pack(queries, keys, values, place):
    seqs, rows, _ = queries.shape
    chips = seqs * KVH
    half = chips // 2
    wide = SHARED * HD
    length = (half - 1) * rows + rows // 2

    def body(place_ref, q_ref, k_ref, v_ref, kv_up, kv_down, q_up, q_down, kv_own, q_own):
        me = place_ref[0]
        for slot in range(chips):
            owner = lax.rem(me + slot, chips)
            seq = owner // KVH
            head = lax.rem(owner, KVH)
            q = q_ref[seq, :, pl.ds(pl.multiple_of(head * wide, wide), wide)]
            k = k_ref[seq, :, pl.ds(pl.multiple_of(head * HD, HD), HD)]
            v = v_ref[seq, :, pl.ds(pl.multiple_of(head * HD, HD), HD)]
            if slot == 0:
                q_own[...] = q
                kv_own[:, :HD] = k
                kv_own[:, HD:] = v
            elif slot == half:
                mid = rows // 2
                at = (half - 1) * rows
                q_up[at:, :] = q[:mid]
                kv_up[at:, :HD] = k[:mid]
                kv_up[at:, HD:] = v[:mid]
                q_down[at:, :] = q[mid:]
                kv_down[at:, :HD] = k[mid:]
                kv_down[at:, HD:] = v[mid:]
            else:
                q_to, kv_to, step = (q_up, kv_up, slot) if slot < half else (q_down, kv_down, chips - slot)
                at = (step - 1) * rows
                q_to[at : at + rows, :] = q
                kv_to[at : at + rows, :HD] = k
                kv_to[at : at + rows, HD:] = v

    long = jax.ShapeDtypeStruct((length, wide), queries.dtype)
    short = jax.ShapeDtypeStruct((rows, wide), queries.dtype)
    return pl.pallas_call(
        body,
        grid=(1,),
        out_shape=(long, long, long, long, short, short),
        in_specs=[smem(), vmem(), vmem(), vmem()],
        out_specs=[vmem()] * 6,
        name="pack",
    )(place, queries, keys, values)


def gather_blocks(q_parts, kv_parts, partner_parts, place, rows, chips):
    half = chips // 2
    wide = SHARED * HD
    count = len(q_parts)
    slots = [0] + [s for k in range(1, half) for s in (k, chips - k)] + [half, half]

    def body(place_ref, *refs):
        q_refs = refs[:count]
        kv_refs = refs[count : 2 * count]
        other_refs = refs[2 * count : 2 * count + len(partner_parts)]
        q_out, k_out, v_out = refs[2 * count + len(partner_parts) :]
        me = place_ref[0]
        core = place_ref[1]
        which, inside = 0, 0
        for i in range(count):
            slot = (chips - slots[i]) % chips
            size = q_parts_rows[i]
            shift = rows // 2 if i == count - 1 else 0
            chunk = lax.rem(me + slot, chips)
            at = pl.multiple_of(chunk * rows + shift, rows // 2)
            for h in range(SHARED):
                q_out[h, pl.ds(at, size), :] = q_refs[i][:size, h * HD : (h + 1) * HD]
            base = pl.multiple_of((chunk * CORES + core) * rows + shift, rows // 2)
            k_out[pl.ds(base, size), :] = kv_refs[i][:size, :HD]
            v_out[pl.ds(base, size), :] = kv_refs[i][:size, HD:]
            if inside >= other_refs[which].shape[0]:
                which, inside = which + 1, 0
            base = pl.multiple_of((chunk * CORES + 1 - core) * rows + shift, rows // 2)
            k_out[pl.ds(base, size), :] = other_refs[which][inside : inside + size, :HD]
            v_out[pl.ds(base, size), :] = other_refs[which][inside : inside + size, HD:]
            inside += size

    q_parts_rows = [rows] * (count - 2) + [rows // 2] * 2
    specs = [first_rows(q_parts_rows[i], wide) for i in range(count)]
    out = (
        jax.ShapeDtypeStruct((SHARED, chips * rows, HD), q_parts[0].dtype),
        jax.ShapeDtypeStruct((chips * CORES * rows, HD), q_parts[0].dtype),
        jax.ShapeDtypeStruct((chips * CORES * rows, HD), q_parts[0].dtype),
    )
    return pl.pallas_call(
        body,
        grid=(1,),
        out_shape=out,
        in_specs=[smem()] + specs + specs + [vmem()] * len(partner_parts),
        out_specs=[vmem()] * 3,
        name="gather_blocks",
    )(place, *q_parts, *kv_parts, *partner_parts)


def attend(q_all, keys, values, place, head, rows, chips):
    half = chips // 2
    tile = TILE_CHUNKS * rows
    span = tile * CORES
    tiles = chips // TILE_CHUNKS
    length = (half - 1) * rows + rows // 2

    def body(place_ref, q_ref, k_ref, v_ref, up, down, own, mixed_ref):
        me = place_ref[0]
        core = place_ref[1]
        valid = place_ref[2]
        row = lax.broadcasted_iota(jnp.int32, (tile, 1), 0)
        offset = (row // rows) * (rows * CORES) + core * rows + lax.rem(row, rows)

        def weights(q, index):
            k = k_ref[pl.ds(pl.multiple_of(index * span, span), span), :]
            score = lax.dot_general(q, k, (((1,), (1,)), ((), ())), preferred_element_type=jnp.float32)
            return jnp.exp2(jnp.tanh(score * tanh_scale) * exp_scale)

        def mix(weight, index):
            v = v_ref[pl.ds(pl.multiple_of(index * span, span), span), :]
            return lax.dot_general(
                weight.astype(jnp.bfloat16), v, (((1,), (0,)), ((), ())), preferred_element_type=jnp.float32
            )

        def one_tile(index, carry):
            first = index * span

            @pl.when(first < valid)
            def _():
                q = q_ref[0, pl.ds(pl.multiple_of(index * tile, tile), tile), :]

                def step(j, state):
                    acc, total = state
                    weight = weights(q, j)
                    return acc + mix(weight, j), total + jnp.sum(weight, axis=1, keepdims=True)

                start = (jnp.zeros((tile, HD), jnp.float32), jnp.zeros((tile, 1), jnp.float32))
                acc, total = lax.fori_loop(0, index, step, start)
                key = lax.broadcasted_iota(jnp.int32, (tile, span), 1)
                weight = jnp.where(key <= offset, weights(q, index), 0.0)
                total = total + jnp.sum(weight, axis=1, keepdims=True)
                acc = acc + mix(weight, index)
                live = first + offset < valid
                result = jnp.where(live, acc / total, 0.0).astype(jnp.bfloat16)
                mixed_ref[pl.ds(pl.multiple_of(index * tile, tile), tile), :] = result

            @pl.when(first >= valid)
            def _():
                mixed_ref[pl.ds(pl.multiple_of(index * tile, tile), tile), :] = jnp.zeros((tile, HD), jnp.bfloat16)

            return carry

        lax.fori_loop(0, tiles, one_tile, 0)
        for slot in range(chips):
            chunk = lax.rem(me + slot, chips)
            block = mixed_ref[pl.ds(pl.multiple_of(chunk * rows, rows), rows), :]
            if slot == 0:
                own[...] = block
            elif slot == half:
                at = (half - 1) * rows
                up[at:, :] = block[: rows // 2]
                down[at:, :] = block[rows // 2 :]
            else:
                to, step = (up, slot) if slot < half else (down, chips - slot)
                to[(step - 1) * rows : step * rows, :] = block

    long = jax.ShapeDtypeStruct((length, HD), q_all.dtype)
    short = jax.ShapeDtypeStruct((rows, HD), q_all.dtype)
    return pl.pallas_call(
        body,
        grid=(1,),
        out_shape=(long, long, short),
        in_specs=[smem(), pl.BlockSpec((1, chips * rows, HD), lambda i: (head, 0, 0)), vmem(), vmem()],
        out_specs=[vmem()] * 3,
        scratch_shapes=[pltpu.VMEM((chips * rows, HD), jnp.bfloat16)],
        name=f"attend_{head}",
    )(place, q_all, keys, values)


def unpack(parts, place, seqs, rows):
    chips = seqs * KVH
    half = chips // 2
    count = len(parts[0])
    slots = [0] + [s for k in range(1, half) for s in (k, chips - k)] + [half, half]
    sizes = [rows] * (count - 2) + [rows // 2] * 2

    def body(place_ref, *refs):
        out = refs[-1]
        me = place_ref[0]
        for i in range(count):
            owner = lax.rem(me + (chips - slots[i]) % chips, chips)
            seq = owner // KVH
            head = lax.rem(owner, KVH)
            start = rows // 2 if i == count - 1 else 0
            for h in range(SHARED):
                at = pl.multiple_of((head * SHARED + h) * HD, HD)
                out[seq, start : start + sizes[i], pl.ds(at, HD)] = refs[h * count + i][...]

    specs = [first_rows(sizes[i], HD) for i in range(count)]
    return pl.pallas_call(
        body,
        grid=(1,),
        out_shape=jax.ShapeDtypeStruct((seqs, rows, HEADS * HD), parts[0][0].dtype),
        in_specs=[smem()] + specs * SHARED,
        out_specs=vmem(),
        name="unpack",
    )(place, *[p for part in parts for p in part])


def shifted(value, by):
    chips = lax.axis_size(RING)
    return lax.ppermute(value, RING, [(i, (i + by) % chips) for i in range(chips)])


def pass_on(chains, rows, each_step=None):
    arrived = [[] for _ in chains]
    rest = list(chains)
    done = []
    step = 0
    while rest[0][0].shape[0]:
        step += 1
        for i in range(len(chains)):
            up, down = rest[i]
            if len(done) >= 3:
                up, down, _ = lax.optimization_barrier((up, down, done[-3]))
            got = lax.optimization_barrier((shifted(up, 1), shifted(down, -1)))
            done.append(got)
            arrived[i].extend(got)
            size = min(rows, up.shape[0])
            rest[i] = tuple(g[size:] for g in got)
        if each_step is not None:
            each_step(step, arrived)
    return arrived


def per_device(queries, keys, values, lengths):
    seqs, rows, _ = queries.shape
    chips = lax.axis_size(RING)
    half = chips // 2
    me = lax.axis_index(RING)
    core = lax.axis_index(CORE)
    valid = lax.dynamic_index_in_dim(lengths, me // KVH, keepdims=False)
    place = jnp.stack([me, core, valid]).astype(jnp.int32)
    kv_up, kv_down, q_up, q_down, kv_own, q_own = pack(queries, keys, values, place)

    swapped = []
    state = {"from": 0}

    def each_step(step, arrived):
        if step not in (half // 3, 2 * half // 3, half - 2, half):
            return
        blocks = ([kv_own] if not swapped else []) + [
            b[: min(rows, b.shape[0])] for b in arrived[0][state["from"] :]
        ]
        state["from"] = len(arrived[0])
        joined = jnp.concatenate(blocks, axis=0)
        swapped.append(lax.ppermute(joined, CORE, [(0, 1), (1, 0)]))

    kv_got, q_got = pass_on([(kv_up, kv_down), (q_up, q_down)], rows, each_step)
    q_all, k_all, v_all = gather_blocks([q_own] + q_got, [kv_own] + kv_got, swapped, place, rows, chips)
    results = [attend(q_all, k_all, v_all, place, h, rows, chips) for h in range(SHARED)]
    back = pass_on([(up, down) for up, down, _ in results], rows)
    parts = [[results[h][2]] + back[h] for h in range(SHARED)]
    return unpack(parts, place, seqs, rows)


def solution(mesh):
    groups = mesh.shape["groups"]
    torus = Mesh(mesh.devices.reshape(groups, -1, CORES), ("groups", RING, CORE))
    placed = P("groups", (RING, CORE), None)
    return jax.shard_map(
        per_device, mesh=torus, in_specs=(placed, placed, placed, P("groups")), out_specs=placed, check_vma=False
    )
```

```python
import functools

import jax
import jax.numpy as jnp
from jax import lax
from jax.experimental import pallas as pl
from jax.experimental.pallas import tpu as pltpu
from jax.sharding import Mesh
from jax.sharding import PartitionSpec as P

HEADS = 32
KVH = 16
HD = 128
SHARED = HEADS // KVH
CORES = 2
RING, CORE = "tp_0", "tp_1"

query_scale = 144.0 ** (-0.5)
soft_cap = 50.0
tanh_scale = query_scale / soft_cap
exp_scale = soft_cap * 1.4426950408889634

TILE_CHUNKS = 8
KEY_SPAN = 512


def vmem():
    return pl.BlockSpec(memory_space=pltpu.VMEM)


def smem():
    return pl.BlockSpec(memory_space=pltpu.SMEM)


def first_rows(count, lanes):
    return pl.BlockSpec((count, lanes), lambda i: (0, 0))


STRIDES = (8, 4, 2, 1)


def whole_rows(array):
    return pl.BlockSpec(array.shape, lambda i: (0, 0))


def piece_of(distance, rows, half):
    if distance < half // 2:
        return 0, (distance - 1) * rows
    return 1, (distance - half // 2) * rows


def buffer_rows(rows, half):
    return (half // 2 - 1) * rows, (half // 2) * rows + rows // 2


def arrivals(rows, half):
    places = []
    sets = [0]
    for number, stride in enumerate(STRIDES):
        sets_now = [o + stride for o in sets]
        places += [(number, i * stride * rows, rows, o) for i, o in enumerate(sets_now)]
        sets = sets + sets_now
    places.append((len(STRIDES), 0, rows // 2, half))
    return places


def pack(queries, keys, values, place):
    seqs, rows, _ = queries.shape
    chips = seqs * KVH
    half = chips // 2
    wide = SHARED * HD
    near, far = buffer_rows(rows, half)

    def body(place_ref, q_ref, k_ref, v_ref, *outs):
        kv_to = (outs[0:2], outs[2:4])
        q_to = (outs[4:6], outs[6:8])
        kv_own, q_own = outs[8:]
        me = place_ref[0]

        def store(kv, qq, at, q, k, v):
            size = q.shape[0]
            qq[at : at + size, :] = q
            kv[at : at + size, :HD] = k
            kv[at : at + size, HD:] = v

        for slot in range(chips):
            owner = lax.rem(me + slot, chips)
            seq = owner // KVH
            head = lax.rem(owner, KVH)
            q = q_ref[seq, :, pl.ds(pl.multiple_of(head * wide, wide), wide)]
            k = k_ref[seq, :, pl.ds(pl.multiple_of(head * HD, HD), HD)]
            v = v_ref[seq, :, pl.ds(pl.multiple_of(head * HD, HD), HD)]
            if slot == 0:
                store(kv_own, q_own, 0, q, k, v)
            elif slot == half:
                mid = rows // 2
                buffer, at = piece_of(half, rows, half)
                store(kv_to[0][buffer], q_to[0][buffer], at, q[:mid], k[:mid], v[:mid])
                store(kv_to[1][buffer], q_to[1][buffer], at, q[mid:], k[mid:], v[mid:])
            else:
                way, distance = (0, slot) if slot < half else (1, chips - slot)
                buffer, at = piece_of(distance, rows, half)
                store(kv_to[way][buffer], q_to[way][buffer], at, q, k, v)

    shapes = [jax.ShapeDtypeStruct((r, wide), queries.dtype) for r in (near, far) * 4 + (rows, rows)]
    out = pl.pallas_call(
        body,
        grid=(1,),
        out_shape=shapes,
        in_specs=[smem(), vmem(), vmem(), vmem()],
        out_specs=[vmem()] * len(shapes),
        name="pack",
    )(place, queries, keys, values)
    return (out[0:2], out[2:4]), (out[4:6], out[6:8]), out[8], out[9]


def gather_blocks(q_own, q_got, kv_own, kv_got, other_own, other_got, place, rows, chips):
    half = chips // 2
    count = len(STRIDES) + 1
    where = arrivals(rows, half)

    def body(place_ref, *refs):
        q_out, k_out, v_out = refs[-3:]
        me = place_ref[0]
        core = place_ref[1]

        def put(q_ref, kv_ref, other_ref, chunk, row, size, shift):
            at = pl.multiple_of(chunk * rows + shift, rows // 2)
            for h in range(SHARED):
                q_out[h, pl.ds(at, size), :] = q_ref[row : row + size, h * HD : (h + 1) * HD]
            for ref, lane, from_row in ((kv_ref, core, row), (other_ref[0], 1 - core, other_ref[1])):
                base = pl.multiple_of((chunk * CORES + lane) * rows + shift, rows // 2)
                k_out[pl.ds(base, size), :] = ref[from_row : from_row + size, :HD]
                v_out[pl.ds(base, size), :] = ref[from_row : from_row + size, HD:]

        put(refs[0], refs[1], (refs[2], 0), me, 0, rows, 0)
        at = 3
        q_refs = refs[at : at + 2 * count]
        kv_refs = refs[at + 2 * count : at + 4 * count]
        early, late = refs[2], refs[at + 4 * count : at + 4 * count + 2]
        inside = rows
        for way in (0, 1):
            for buffer, row, size, distance in where:
                shift = rows // 2 if distance == half and way else 0
                slot = (chips - distance) % chips if way == 0 else distance
                chunk = lax.rem(me + slot, chips)
                if buffer == len(STRIDES) - 1:
                    other = (late[way], row)
                else:
                    other = (early, inside)
                    inside += size
                index = way * count + buffer
                put(q_refs[index], kv_refs[index], other, chunk, row, size, shift)

    args = [q_own, kv_own, other_own, *q_got[0], *q_got[1], *kv_got[0], *kv_got[1], *other_got]
    out = (
        jax.ShapeDtypeStruct((SHARED, chips * rows, HD), q_own.dtype),
        jax.ShapeDtypeStruct((chips * CORES * rows, HD), q_own.dtype),
        jax.ShapeDtypeStruct((chips * CORES * rows, HD), q_own.dtype),
    )
    return pl.pallas_call(
        body,
        grid=(1,),
        out_shape=out,
        in_specs=[smem()] + [vmem()] * len(args),
        out_specs=[vmem()] * 3,
        name="gather_blocks",
    )(place, *args)


def attend(q_all, keys, values, place, head, rows, chips, token):
    half = chips // 2
    tile = TILE_CHUNKS * rows
    span = KEY_SPAN
    tiles = chips // TILE_CHUNKS
    near, far = buffer_rows(rows, half)

    def body(place_ref, q_ref, k_ref, v_ref, _, *outs):
        to = (outs[0:2], outs[2:4])
        own, mixed_ref = outs[4:]
        me = place_ref[0]
        core = place_ref[1]
        valid = place_ref[2]
        row = lax.broadcasted_iota(jnp.int32, (tile, 1), 0)
        offset = (row // rows) * (rows * CORES) + core * rows + lax.rem(row, rows)

        def weights(q, at):
            k = k_ref[pl.ds(at, span), :]
            score = lax.dot_general(q, k, (((1,), (1,)), ((), ())), preferred_element_type=jnp.float32)
            return jnp.exp2(jnp.tanh(score * tanh_scale) * exp_scale)

        def mix(weight, at):
            v = v_ref[pl.ds(at, span), :]
            return lax.dot_general(
                weight.astype(jnp.bfloat16), v, (((1,), (0,)), ((), ())), preferred_element_type=jnp.float32
            )

        def by_lane(weight):
            total = weight[:, :HD]
            for at in range(HD, span, HD):
                total = total + weight[:, at : at + HD]
            return total

        def one_tile(index, carry):
            first = index * tile * CORES

            @pl.when(first < valid)
            def _():
                q = q_ref[0, pl.ds(pl.multiple_of(index * tile, tile), tile), :]

                def step(j, state):
                    acc, total = state
                    for at in range(0, tile * CORES, span):
                        start = pl.multiple_of(j * tile * CORES + at, span)
                        weight = weights(q, start)
                        acc = acc + mix(weight, start)
                        total = total + by_lane(weight)
                    return acc, total

                zero = jnp.zeros((tile, HD), jnp.float32)
                acc, total = lax.fori_loop(0, index, step, (zero, zero))
                for at in range(0, tile * CORES, span):
                    start = pl.multiple_of(first + at, span)
                    key = lax.broadcasted_iota(jnp.int32, (tile, span), 1) + at
                    weight = jnp.where(key <= offset, weights(q, start), 0.0)
                    acc = acc + mix(weight, start)
                    total = total + by_lane(weight)
                live = first + offset < valid
                result = jnp.where(live, acc / jnp.sum(total, axis=1, keepdims=True), 0.0).astype(jnp.bfloat16)
                mixed_ref[pl.ds(pl.multiple_of(index * tile, tile), tile), :] = result

            @pl.when(first >= valid)
            def _():
                mixed_ref[pl.ds(pl.multiple_of(index * tile, tile), tile), :] = jnp.zeros((tile, HD), jnp.bfloat16)

            return carry

        lax.fori_loop(0, tiles, one_tile, 0)
        for slot in range(chips):
            chunk = lax.rem(me + slot, chips)
            block = mixed_ref[pl.ds(pl.multiple_of(chunk * rows, rows), rows), :]
            if slot == 0:
                own[...] = block
            elif slot == half:
                buffer, at = piece_of(half, rows, half)
                to[0][buffer][at:, :] = block[: rows // 2]
                to[1][buffer][at:, :] = block[rows // 2 :]
            else:
                way, distance = (0, slot) if slot < half else (1, chips - slot)
                buffer, at = piece_of(distance, rows, half)
                to[way][buffer][at : at + rows, :] = block

    shapes = [jax.ShapeDtypeStruct((r, HD), q_all.dtype) for r in (near, far, near, far, rows)]
    out = pl.pallas_call(
        body,
        grid=(1,),
        out_shape=shapes,
        in_specs=[smem(), pl.BlockSpec((1, chips * rows, HD), lambda i: (head, 0, 0)), vmem(), vmem(), vmem()],
        out_specs=[vmem()] * len(shapes),
        scratch_shapes=[pltpu.VMEM((chips * rows, HD), jnp.bfloat16)],
        cost_estimate=pl.CostEstimate(
            flops=2 * (chips * rows) ** 2 * CORES * HD,
            transcendentals=(chips * rows) ** 2 * CORES,
            bytes_accessed=6 * chips * rows * HD * 2,
        ),
        name=f"attend_{head}",
    )(place, q_all, keys, values, token)
    return (out[0:2], out[2:4]), out[4]


def unpack(owns, parts, place, seqs, rows):
    chips = seqs * KVH
    half = chips // 2
    count = len(STRIDES) + 1
    where = arrivals(rows, half)

    def body(place_ref, *refs):
        out = refs[-1]
        me = place_ref[0]

        def put(ref, h, owner, row, size, start):
            seq = owner // KVH
            head = lax.rem(owner, KVH)
            at = pl.multiple_of((head * SHARED + h) * HD, HD)
            out[seq, start : start + size, pl.ds(at, HD)] = ref[row : row + size, :]

        for h in range(SHARED):
            mine = refs[h * (2 * count + 1) : (h + 1) * (2 * count + 1)]
            put(mine[0], h, me, 0, rows, 0)
            for way in (0, 1):
                for buffer, row, size, distance in where:
                    start = rows // 2 if distance == half and way else 0
                    slot = (chips - distance) % chips if way == 0 else distance
                    put(mine[1 + way * count + buffer], h, lax.rem(me + slot, chips), row, size, start)

    args = [a for own, part in zip(owns, parts) for a in (own, *part[0], *part[1])]
    return pl.pallas_call(
        body,
        grid=(1,),
        out_shape=jax.ShapeDtypeStruct((seqs, rows, HEADS * HD), owns[0].dtype),
        in_specs=[smem()] + [vmem()] * len(args),
        out_specs=vmem(),
        name="unpack",
    )(place, *args)


def shifted(value, by):
    chips = lax.axis_size(RING)
    return lax.ppermute(value, RING, [(i, (i + by) % chips) for i in range(chips)])


def stage_blocks(near, arrived, stride, rows, half, token, name):
    spans = []
    for way in (0, 1):
        mine = [(0, (stride - 1) * rows, stride * rows)]
        for index, before in enumerate(STRIDES[: len(arrived[way])]):
            mine += [(index + 1, at + stride * rows, stride * rows) for at in range(0, half // 2 * rows, before * rows)]
        spans.append(mine)
    per = 1 + len(arrived[0])
    extra = len(arrived[0]) == 1
    size = half // 2 * rows
    lanes = near[0].shape[1]

    def body(*refs):
        token_ref = refs[2 * per]
        outs = refs[2 * per + 1 :]
        for way in (0, 1):
            mine = refs[way * per : (way + 1) * per]
            at = 0
            for index, row, count in spans[way]:
                outs[way][at : at + count, :] = mine[index][row : row + count, :]
                at += count
            if extra:
                outs[2 + way][...] = mine[1][size:, :]
        outs[-1][...] = token_ref[...]

    shapes = [jax.ShapeDtypeStruct((size, lanes), near[0].dtype)] * 2
    if extra:
        shapes += [jax.ShapeDtypeStruct((rows // 2, lanes), near[0].dtype)] * 2
    shapes.append(jax.ShapeDtypeStruct(token.shape, token.dtype))
    args = [near[0], *arrived[0], near[1], *arrived[1], token]
    out = pl.pallas_call(
        body,
        grid=(1,),
        out_shape=shapes,
        in_specs=[vmem()] * len(args),
        out_specs=[vmem()] * len(shapes),
        name=name,
    )(*args)
    return out[:-1], out[-1]


def spread(chains, rows, half, token, each_stage=None):
    arrived = [([], []) for _ in chains]
    extras = [None] * len(chains)
    for number, stride in enumerate(STRIDES):
        for i, chain in enumerate(chains):
            if number == 0:
                sends = (chain[0][1], chain[1][1])
            else:
                near = (chain[0][0], chain[1][0])
                sends, token = stage_blocks(near, arrived[i], stride, rows, half, token, f"stage_{stride}_{i}")
            got = shifted(sends[0], stride), shifted(sends[1], -stride)
            if number == 1:
                extras[i] = shifted(sends[2], half // 2), shifted(sends[3], -(half // 2))
            for way in (0, 1):
                arrived[i][way].append(got[way])
            if each_stage is not None:
                each_stage(number, i, arrived[i], extras[i])
    return [(up + [extras[i][0]], down + [extras[i][1]]) for i, (up, down) in enumerate(arrived)], token


def early_blocks(own, got, where, token):
    last = len(STRIDES) - 1
    picks = [(way, b, row, size) for way in (0, 1) for b, row, size, _ in where if b != last]
    count = own.shape[0] + sum(p[3] for p in picks)
    parts = [got[way][b] for way in (0, 1) for b in range(last + 2) if b != last]

    def body(own_ref, *refs):
        out = refs[-1]
        out[: own.shape[0], :] = own_ref[...]
        at = own.shape[0]
        for way, b, row, size in picks:
            ref = refs[way * (last + 1) + (b if b < last else last)]
            out[at : at + size, :] = ref[row : row + size, :]
            at += size

    joined = pl.pallas_call(
        body,
        grid=(1,),
        out_shape=jax.ShapeDtypeStruct((count, own.shape[1]), own.dtype),
        in_specs=[vmem()] * (len(parts) + 1),
        out_specs=vmem(),
        name="early_blocks",
    )(own, *parts)
    return joined, token


def per_device(queries, keys, values, lengths):
    seqs, rows, _ = queries.shape
    chips = lax.axis_size(RING)
    half = chips // 2
    me = lax.axis_index(RING)
    core = lax.axis_index(CORE)
    valid = jnp.sum(jnp.where(jnp.arange(seqs) == me // KVH, lengths, 0))
    place = jnp.stack([me, core, valid]).astype(jnp.int32)
    kv, q, kv_own, q_own = pack(queries, keys, values, place)

    def swap(value):
        return lax.ppermute(value, CORE, [(0, 1), (1, 0)])

    token = kv_own[:8, :HD]
    (kv_got, q_got), token = spread((kv, q), rows, half, token)
    where = arrivals(rows, half)
    early, token = early_blocks(kv_own, kv_got, where, token)
    other_early = swap(early)
    other_late = [swap(kv_got[way][len(STRIDES) - 1]) for way in (0, 1)]
    q_all, k_all, v_all = gather_blocks(q_own, q_got, kv_own, kv_got, other_early, other_late, place, rows, chips)
    results = []
    token = q_own[:8]
    for h in range(SHARED):
        results.append(attend(q_all, k_all, v_all, place, h, rows, chips, token))
        token = results[-1][1][:8]
    back, _ = spread([r[0] for r in results], rows, half, results[1][1][:8])
    return unpack([r[1] for r in results], back, place, seqs, rows)


def solution(mesh):
    groups = mesh.shape["groups"]
    torus = Mesh(mesh.devices.reshape(groups, -1, CORES), ("groups", RING, CORE))
    placed = P("groups", (RING, CORE), None)
    return jax.shard_map(
        per_device, mesh=torus, in_specs=(placed, placed, placed, P("groups")), out_specs=placed, check_vma=False
    )
```

```python
import jax
import jax.numpy as jnp
from jax import lax
from jax.experimental import pallas as pl
from jax.experimental.pallas import tpu as pltpu
from jax.sharding import Mesh
from jax.sharding import PartitionSpec as P

HEADS = 32
KVH = 16
HD = 128
SHARED = HEADS // KVH
WIDE = SHARED * HD
CORES = 2
RING, CORE = "tp_0", "tp_1"

query_scale = 144.0 ** (-0.5)
soft_cap = 50.0
tanh_scale = query_scale / soft_cap
exp_scale = soft_cap * 1.4426950408889634

TILE = 1024
SPAN = 256
UNROLL = 2
PART = 256


def vmem():
    return pl.BlockSpec(memory_space=pltpu.VMEM)


def smem():
    return pl.BlockSpec(memory_space=pltpu.SMEM)


def pack(queries, keys, values):
    seqs, rows, _ = queries.shape

    def body(q_ref, k_ref, v_ref, out):
        for seq in range(seqs):
            for head in range(KVH):
                at = (seq * KVH + head) * rows
                out[at : at + rows, :WIDE] = q_ref[seq, :, head * WIDE : (head + 1) * WIDE]
                out[at : at + rows, WIDE : WIDE + HD] = k_ref[seq, :, head * HD : (head + 1) * HD]
                out[at : at + rows, WIDE + HD :] = v_ref[seq, :, head * HD : (head + 1) * HD]

    return pl.pallas_call(
        body,
        grid=(1,),
        out_shape=jax.ShapeDtypeStruct((seqs * KVH * rows, WIDE + 2 * HD), queries.dtype),
        in_specs=[vmem()] * 3,
        out_specs=vmem(),
        name="pack",
    )(queries, keys, values)


def attend(mine, other, place, rows):
    length = mine.shape[0]
    tiles = length // TILE

    def body(place_ref, x_ref, y_ref, out):
        core = place_ref[0]
        valid = place_ref[1]

        def weights(q, ref, at, lane, size):
            k = ref[pl.ds(at, size), lane : lane + HD]
            score = lax.dot_general(q, k, (((1,), (1,)), ((), ())), preferred_element_type=jnp.float32)
            return jnp.exp2(jnp.tanh(score * tanh_scale) * exp_scale)

        def mix(weight, ref, at, lane, size):
            v = ref[pl.ds(at, size), lane : lane + HD]
            return lax.dot_general(
                weight.astype(jnp.bfloat16), v, (((1,), (0,)), ((), ())), preferred_element_type=jnp.float32
            )

        def by_lane(weight):
            total = weight[:, :HD]
            for at in range(HD, weight.shape[1], HD):
                total = total + weight[:, at : at + HD]
            return total

        sources = ((x_ref, WIDE), (y_ref, 0))

        def one_tile(index, carry):
            first = pl.multiple_of(index * TILE, TILE)

            @pl.when(first * CORES < valid)
            def _():
                qs = [x_ref[pl.ds(first, TILE), h * HD : (h + 1) * HD] for h in range(SHARED)]

                def step(j, state):
                    state = [list(s) for s in state]
                    for u in range(UNROLL):
                        at = pl.multiple_of((j * UNROLL + u) * SPAN, SPAN)
                        for ref, lane in sources:
                            for h in range(SHARED):
                                weight = weights(qs[h], ref, at, lane, SPAN)
                                state[h][0] = state[h][0] + mix(weight, ref, at, lane + HD, SPAN)
                                state[h][1] = state[h][1] + by_lane(weight)
                    return tuple(tuple(s) for s in state)

                zero = jnp.zeros((TILE, HD), jnp.float32)
                state = lax.fori_loop(0, index * (TILE // (SPAN * UNROLL)), step, ((zero, zero),) * SHARED)
                for at in range(0, TILE, PART):
                    row = lax.broadcasted_iota(jnp.int32, (PART, 1), 0) + at
                    token = (row // rows) * (rows * CORES) + core * rows + lax.rem(row, rows)
                    live = first * CORES + token < valid
                    limits = (row, (row // rows + core) * rows - 1)
                    size = at + PART
                    key = lax.broadcasted_iota(jnp.int32, (PART, size), 1)
                    for h in range(SHARED):
                        acc = state[h][0][at:size]
                        total = state[h][1][at:size]
                        for (ref, lane), limit in zip(sources, limits):
                            weight = weights(qs[h][at:size], ref, first, lane, size)
                            weight = jnp.where(key <= limit, weight, 0.0)
                            acc = acc + mix(weight, ref, first, lane + HD, size)
                            total = total + by_lane(weight)
                        result = acc / jnp.sum(total, axis=1, keepdims=True)
                        result = jnp.where(live, result, 0.0).astype(jnp.bfloat16)
                        out[pl.ds(pl.multiple_of(first + at, PART), PART), h * HD : (h + 1) * HD] = result

            @pl.when(first * CORES >= valid)
            def _():
                out[pl.ds(first, TILE), :] = jnp.zeros((TILE, WIDE), jnp.bfloat16)

            return carry

        lax.fori_loop(0, tiles, one_tile, 0)

    return pl.pallas_call(
        body,
        grid=(1,),
        out_shape=jax.ShapeDtypeStruct((length, WIDE), mine.dtype),
        in_specs=[smem(), vmem(), vmem()],
        out_specs=vmem(),
        name="attend",
    )(place, mine, other)


def per_device(queries, keys, values, lengths):
    seqs, rows, _ = queries.shape
    core = lax.axis_index(CORE)
    own_seq = lax.axis_index(RING) // KVH
    valid = jnp.sum(jnp.where(jnp.arange(seqs) == own_seq, lengths, 0))
    place = jnp.stack([core, valid]).astype(jnp.int32)
    blocks = pack(queries, keys, values)
    mine = lax.all_to_all(blocks, RING, 0, 0, tiled=True)
    other = lax.ppermute(mine[:, WIDE:], CORE, [(i, CORES - 1 - i) for i in range(CORES)])
    output = attend(mine, other, place, rows)
    back = lax.all_to_all(output, RING, 0, 0, tiled=True)
    return back.reshape(seqs, KVH, rows, WIDE).transpose(0, 2, 1, 3).reshape(seqs, rows, HEADS * HD)


def solution(mesh):
    groups = mesh.shape["groups"]
    torus = Mesh(mesh.devices.reshape(groups, -1, CORES), ("groups", RING, CORE))
    placed = P("groups", (RING, CORE), None)
    return jax.shard_map(
        per_device, mesh=torus, in_specs=(placed, placed, placed, P("groups")), out_specs=placed, check_vma=False
    )
```

```python
import jax
import jax.numpy as jnp
from jax import lax
from jax.experimental import pallas as pl
from jax.experimental.pallas import tpu as pltpu
from jax.sharding import Mesh
from jax.sharding import PartitionSpec as P

HEADS = 32
KVH = 16
HD = 128
SHARED = HEADS // KVH
WIDE = SHARED * HD
CORES = 2
RING, CORE = "tp_0", "tp_1"

query_scale = 144.0 ** (-0.5)
soft_cap = 50.0
tanh_scale = query_scale / soft_cap
exp_scale = soft_cap * 1.4426950408889634

TILE = 1024
SPAN = 256
UNROLL = 2
PART = 256
STEPS = 2
ROOM = 40 * 1024 * 1024


def vmem():
    return pl.BlockSpec(memory_space=pltpu.VMEM)


def smem():
    return pl.BlockSpec(memory_space=pltpu.SMEM)


def pack(queries, keys, values):
    seqs, rows, _ = queries.shape
    few = KVH // STEPS

    def body(q_ref, k_ref, v_ref, out):
        for head in range(few):
            at = head * rows
            out[at : at + rows, :WIDE] = q_ref[0, :, head * WIDE : (head + 1) * WIDE]
            out[at : at + rows, WIDE : WIDE + HD] = k_ref[0, :, head * HD : (head + 1) * HD]
            out[at : at + rows, WIDE + HD :] = v_ref[0, :, head * HD : (head + 1) * HD]

    def cut(width):
        return pl.BlockSpec((1, rows, few * width), lambda s, i: (s, 0, i))

    return pl.pallas_call(
        body,
        grid=(seqs, STEPS),
        out_shape=jax.ShapeDtypeStruct((seqs * KVH * rows, WIDE + 2 * HD), queries.dtype),
        in_specs=[cut(WIDE), cut(HD), cut(HD)],
        out_specs=pl.BlockSpec((few * rows, WIDE + 2 * HD), lambda s, i: (s * STEPS + i, 0)),
        name="pack",
    )(queries, keys, values)


def unpack(blocks, seqs, rows):
    few = KVH // STEPS

    def body(x_ref, out):
        for head in range(few):
            out[0, :, head * WIDE : (head + 1) * WIDE] = x_ref[head * rows : (head + 1) * rows, :]

    return pl.pallas_call(
        body,
        grid=(seqs, STEPS),
        out_shape=jax.ShapeDtypeStruct((seqs, rows, KVH * WIDE), blocks.dtype),
        in_specs=[pl.BlockSpec((few * rows, WIDE), lambda s, i: (s * STEPS + i, 0))],
        out_specs=pl.BlockSpec((1, rows, few * WIDE), lambda s, i: (s, 0, i)),
        compiler_params=pltpu.CompilerParams(vmem_limit_bytes=ROOM),
        name="unpack",
    )(blocks)


def attend(mine, other, place, rows):
    length = mine.shape[0]
    tiles = length // TILE

    def body(place_ref, x_ref, y_ref, out):
        core = place_ref[0]
        valid = place_ref[1]

        def weights(q, ref, at, lane, size):
            k = ref[pl.ds(at, size), lane : lane + HD]
            score = lax.dot_general(q, k, (((1,), (1,)), ((), ())), preferred_element_type=jnp.float32)
            return jnp.exp2(jnp.tanh(score * tanh_scale) * exp_scale)

        def mix(weight, ref, at, lane, size):
            v = ref[pl.ds(at, size), lane : lane + HD]
            return lax.dot_general(
                weight.astype(jnp.bfloat16), v, (((1,), (0,)), ((), ())), preferred_element_type=jnp.float32
            )

        def by_lane(weight):
            total = weight[:, :HD]
            for at in range(HD, weight.shape[1], HD):
                total = total + weight[:, at : at + HD]
            return total

        sources = ((x_ref, WIDE), (y_ref, 0))

        def one_tile(index, carry):
            first = pl.multiple_of(index * TILE, TILE)

            @pl.when(first * CORES < valid)
            def _():
                qs = [x_ref[pl.ds(first, TILE), h * HD : (h + 1) * HD] for h in range(SHARED)]

                def step(j, state):
                    state = [list(s) for s in state]
                    for u in range(UNROLL):
                        at = pl.multiple_of((j * UNROLL + u) * SPAN, SPAN)
                        for ref, lane in sources:
                            for h in range(SHARED):
                                weight = weights(qs[h], ref, at, lane, SPAN)
                                state[h][0] = state[h][0] + mix(weight, ref, at, lane + HD, SPAN)
                                state[h][1] = state[h][1] + by_lane(weight)
                    return tuple(tuple(s) for s in state)

                zero = jnp.zeros((TILE, HD), jnp.float32)
                state = lax.fori_loop(0, index * (TILE // (SPAN * UNROLL)), step, ((zero, zero),) * SHARED)
                for at in range(0, TILE, PART):
                    row = lax.broadcasted_iota(jnp.int32, (PART, 1), 0) + at
                    token = (row // rows) * (rows * CORES) + core * rows + lax.rem(row, rows)
                    live = first * CORES + token < valid
                    limits = (row, (row // rows + core) * rows - 1)
                    size = at + PART
                    key = lax.broadcasted_iota(jnp.int32, (PART, size), 1)
                    for h in range(SHARED):
                        acc = state[h][0][at:size]
                        total = state[h][1][at:size]
                        for (ref, lane), limit in zip(sources, limits):
                            weight = weights(qs[h][at:size], ref, first, lane, size)
                            weight = jnp.where(key <= limit, weight, 0.0)
                            acc = acc + mix(weight, ref, first, lane + HD, size)
                            total = total + by_lane(weight)
                        result = acc / jnp.sum(total, axis=1, keepdims=True)
                        result = jnp.where(live, result, 0.0).astype(jnp.bfloat16)
                        out[pl.ds(pl.multiple_of(first + at, PART), PART), h * HD : (h + 1) * HD] = result

            @pl.when(first * CORES >= valid)
            def _():
                out[pl.ds(first, TILE), :] = jnp.zeros((TILE, WIDE), jnp.bfloat16)

            return carry

        lax.fori_loop(0, tiles, one_tile, 0)

    return pl.pallas_call(
        body,
        out_shape=jax.ShapeDtypeStruct((length, WIDE), mine.dtype),
        in_specs=[smem(), vmem(), vmem()],
        out_specs=vmem(),
        compiler_params=pltpu.CompilerParams(vmem_limit_bytes=ROOM),
        name="attend",
    )(place, mine, other)


def per_device(queries, keys, values, lengths):
    seqs, rows, _ = queries.shape
    core = lax.axis_index(CORE)
    own_seq = lax.axis_index(RING) // KVH
    valid = jnp.sum(jnp.where(jnp.arange(seqs) == own_seq, lengths, 0))
    place = jnp.stack([core, valid]).astype(jnp.int32)
    blocks = pack(queries, keys, values)
    mine = lax.all_to_all(blocks, RING, 0, 0, tiled=True)
    other = lax.ppermute(mine[:, WIDE:], CORE, [(i, CORES - 1 - i) for i in range(CORES)])
    output = attend(mine, other, place, rows)
    back = lax.all_to_all(output, RING, 0, 0, tiled=True)
    return unpack(back, seqs, rows)


def solution(mesh):
    groups = mesh.shape["groups"]
    torus = Mesh(mesh.devices.reshape(groups, -1, CORES), ("groups", RING, CORE))
    placed = P("groups", (RING, CORE), None)
    return jax.shard_map(
        per_device, mesh=torus, in_specs=(placed, placed, placed, P("groups")), out_specs=placed, check_vma=False
    )
```

```python
import jax
import jax.numpy as jnp
from jax import lax
from jax.experimental import pallas as pl
from jax.experimental.pallas import tpu as pltpu
from jax.sharding import Mesh
from jax.sharding import PartitionSpec as P

HEADS = 32
KVH = 16
HD = 128
SHARED = HEADS // KVH
WIDE = SHARED * HD
CORES = 2
RING, CORE = "tp_0", "tp_1"

query_scale = 144.0 ** (-0.5)
soft_cap = 50.0
tanh_scale = query_scale / soft_cap
exp_scale = soft_cap * 1.4426950408889634

TILE = 1024
SPAN = 256
UNROLL = 4
PART = 256
STEPS = 2
ROOM = 40 * 1024 * 1024


def vmem():
    return pl.BlockSpec(memory_space=pltpu.VMEM)


def smem():
    return pl.BlockSpec(memory_space=pltpu.SMEM)


def pack(queries, keys, values):
    seqs, rows, _ = queries.shape

    def body(q_ref, k_ref, v_ref, out):
        for seq in range(seqs):
            for head in range(KVH):
                at = (seq * KVH + head) * rows
                out[at : at + rows, :WIDE] = q_ref[seq, :, head * WIDE : (head + 1) * WIDE]
                out[at : at + rows, WIDE : WIDE + HD] = k_ref[seq, :, head * HD : (head + 1) * HD]
                out[at : at + rows, WIDE + HD :] = v_ref[seq, :, head * HD : (head + 1) * HD]

    return pl.pallas_call(
        body,
        grid=(1,),
        out_shape=jax.ShapeDtypeStruct((seqs * KVH * rows, WIDE + 2 * HD), queries.dtype),
        in_specs=[vmem()] * 3,
        out_specs=vmem(),
        name="pack",
    )(queries, keys, values)


def unpack(blocks, seqs, rows):
    few = KVH // STEPS

    def body(x_ref, out):
        for head in range(few):
            out[0, :, head * WIDE : (head + 1) * WIDE] = x_ref[head * rows : (head + 1) * rows, :]

    return pl.pallas_call(
        body,
        grid=(seqs, STEPS),
        out_shape=jax.ShapeDtypeStruct((seqs, rows, KVH * WIDE), blocks.dtype),
        in_specs=[pl.BlockSpec((few * rows, WIDE), lambda s, i: (s * STEPS + i, 0))],
        out_specs=pl.BlockSpec((1, rows, few * WIDE), lambda s, i: (s, 0, i)),
        compiler_params=pltpu.CompilerParams(vmem_limit_bytes=ROOM),
        name="unpack",
    )(blocks)


def attend(mine, other, place, rows):
    length = mine.shape[0]
    tiles = length // TILE

    def body(place_ref, x_ref, y_ref, out):
        core = place_ref[0]
        valid = place_ref[1]

        def weights(q, ref, at, lane, size):
            k = ref[pl.ds(at, size), lane : lane + HD]
            score = lax.dot_general(q, k, (((1,), (1,)), ((), ())), preferred_element_type=jnp.float32)
            return jnp.exp2(jnp.tanh(score * tanh_scale) * exp_scale)

        def mix(weight, ref, at, lane, size):
            v = ref[pl.ds(at, size), lane : lane + HD]
            return lax.dot_general(
                weight.astype(jnp.bfloat16), v, (((1,), (0,)), ((), ())), preferred_element_type=jnp.float32
            )

        def by_lane(weight):
            total = weight[:, :HD]
            for at in range(HD, weight.shape[1], HD):
                total = total + weight[:, at : at + HD]
            return total

        sources = ((x_ref, WIDE), (y_ref, 0))

        def one_tile(index, carry):
            first = pl.multiple_of(index * TILE, TILE)

            @pl.when(first * CORES < valid)
            def _():
                qs = [x_ref[pl.ds(first, TILE), h * HD : (h + 1) * HD] for h in range(SHARED)]

                def step(j, state):
                    state = [list(s) for s in state]
                    for u in range(UNROLL):
                        at = pl.multiple_of((j * UNROLL + u) * SPAN, SPAN)
                        for ref, lane in sources:
                            for h in range(SHARED):
                                weight = weights(qs[h], ref, at, lane, SPAN)
                                state[h][0] = state[h][0] + mix(weight, ref, at, lane + HD, SPAN)
                                state[h][1] = state[h][1] + by_lane(weight)
                    return tuple(tuple(s) for s in state)

                zero = jnp.zeros((TILE, HD), jnp.float32)
                state = lax.fori_loop(0, index * (TILE // (SPAN * UNROLL)), step, ((zero, zero),) * SHARED)
                for at in range(0, TILE, PART):
                    row = lax.broadcasted_iota(jnp.int32, (PART, 1), 0) + at
                    token = (row // rows) * (rows * CORES) + core * rows + lax.rem(row, rows)
                    live = first * CORES + token < valid
                    limits = (row, (row // rows + core) * rows - 1)
                    size = at + PART
                    key = lax.broadcasted_iota(jnp.int32, (PART, size), 1)
                    for h in range(SHARED):
                        acc = state[h][0][at:size]
                        total = state[h][1][at:size]
                        for (ref, lane), limit in zip(sources, limits):
                            weight = weights(qs[h][at:size], ref, first, lane, size)
                            weight = jnp.where(key <= limit, weight, 0.0)
                            acc = acc + mix(weight, ref, first, lane + HD, size)
                            total = total + by_lane(weight)
                        result = acc / jnp.sum(total, axis=1, keepdims=True)
                        result = jnp.where(live, result, 0.0).astype(jnp.bfloat16)
                        out[pl.ds(pl.multiple_of(first + at, PART), PART), h * HD : (h + 1) * HD] = result

            @pl.when(first * CORES >= valid)
            def _():
                out[pl.ds(first, TILE), :] = jnp.zeros((TILE, WIDE), jnp.bfloat16)

            return carry

        lax.fori_loop(0, tiles, one_tile, 0)

    return pl.pallas_call(
        body,
        out_shape=jax.ShapeDtypeStruct((length, WIDE), mine.dtype),
        in_specs=[smem(), vmem(), vmem()],
        out_specs=vmem(),
        compiler_params=pltpu.CompilerParams(vmem_limit_bytes=ROOM),
        name="attend",
    )(place, mine, other)


def per_device(queries, keys, values, lengths):
    seqs, rows, _ = queries.shape
    core = lax.axis_index(CORE)
    own_seq = lax.axis_index(RING) // KVH
    valid = jnp.sum(jnp.where(jnp.arange(seqs) == own_seq, lengths, 0))
    place = jnp.stack([core, valid]).astype(jnp.int32)
    blocks = pack(queries, keys, values)
    mine = lax.all_to_all(blocks, RING, 0, 0, tiled=True)
    other = lax.ppermute(mine[:, WIDE:], CORE, [(i, CORES - 1 - i) for i in range(CORES)])
    output = attend(mine, other, place, rows)
    back = lax.all_to_all(output, RING, 0, 0, tiled=True)
    return unpack(back, seqs, rows)


def solution(mesh):
    groups = mesh.shape["groups"]
    torus = Mesh(mesh.devices.reshape(groups, -1, CORES), ("groups", RING, CORE))
    placed = P("groups", (RING, CORE), None)
    return jax.shard_map(
        per_device, mesh=torus, in_specs=(placed, placed, placed, P("groups")), out_specs=placed, check_vma=False
    )
```

```python
import jax
import jax.numpy as jnp
from jax import lax
from jax.experimental import pallas as pl
from jax.experimental.pallas import tpu as pltpu
from jax.sharding import Mesh
from jax.sharding import PartitionSpec as P

HEADS = 32
KVH = 16
HD = 128
SHARED = HEADS // KVH
WIDE = SHARED * HD
CORES = 2
RING, CORE = "tp_0", "tp_1"

query_scale = 144.0 ** (-0.5)
soft_cap = 50.0
tanh_scale = query_scale / soft_cap
exp_scale = soft_cap * 1.4426950408889634

TILE = 1024
SPAN = 512
UNROLL = 2
PART = 256
STEPS = 2
ROOM = 40 * 1024 * 1024


def vmem():
    return pl.BlockSpec(memory_space=pltpu.VMEM)


def smem():
    return pl.BlockSpec(memory_space=pltpu.SMEM)


def pack(queries, keys, values):
    seqs, rows, _ = queries.shape

    def body(q_ref, k_ref, v_ref, out):
        for seq in range(seqs):
            for head in range(KVH):
                at = (seq * KVH + head) * rows
                out[at : at + rows, :WIDE] = q_ref[seq, :, head * WIDE : (head + 1) * WIDE]
                out[at : at + rows, WIDE : WIDE + HD] = k_ref[seq, :, head * HD : (head + 1) * HD]
                out[at : at + rows, WIDE + HD :] = v_ref[seq, :, head * HD : (head + 1) * HD]

    return pl.pallas_call(
        body,
        grid=(1,),
        out_shape=jax.ShapeDtypeStruct((seqs * KVH * rows, WIDE + 2 * HD), queries.dtype),
        in_specs=[vmem()] * 3,
        out_specs=vmem(),
        name="pack",
    )(queries, keys, values)


def unpack(blocks, seqs, rows):
    few = KVH // STEPS

    def body(x_ref, out):
        for head in range(few):
            out[0, :, head * WIDE : (head + 1) * WIDE] = x_ref[head * rows : (head + 1) * rows, :]

    return pl.pallas_call(
        body,
        grid=(seqs, STEPS),
        out_shape=jax.ShapeDtypeStruct((seqs, rows, KVH * WIDE), blocks.dtype),
        in_specs=[pl.BlockSpec((few * rows, WIDE), lambda s, i: (s * STEPS + i, 0))],
        out_specs=pl.BlockSpec((1, rows, few * WIDE), lambda s, i: (s, 0, i)),
        compiler_params=pltpu.CompilerParams(vmem_limit_bytes=ROOM),
        name="unpack",
    )(blocks)


def attend(mine, other, place, rows):
    length = mine.shape[0]
    tiles = length // TILE

    def body(place_ref, x_ref, y_ref, out):
        core = place_ref[0]
        valid = place_ref[1]

        def weights(q, ref, at, lane, size):
            k = ref[pl.ds(at, size), lane : lane + HD]
            score = lax.dot_general(q, k, (((1,), (1,)), ((), ())), preferred_element_type=jnp.float32)
            return jnp.exp2(jnp.tanh(score * tanh_scale) * exp_scale)

        def mix(weight, ref, at, lane, size):
            v = ref[pl.ds(at, size), lane : lane + HD]
            return lax.dot_general(
                weight.astype(jnp.bfloat16), v, (((1,), (0,)), ((), ())), preferred_element_type=jnp.float32
            )

        def by_lane(weight):
            total = weight[:, :HD]
            for at in range(HD, weight.shape[1], HD):
                total = total + weight[:, at : at + HD]
            return total

        sources = ((x_ref, WIDE), (y_ref, 0))

        def one_tile(index, carry):
            first = pl.multiple_of(index * TILE, TILE)

            @pl.when(first * CORES < valid)
            def _():
                qs = [x_ref[pl.ds(first, TILE), h * HD : (h + 1) * HD] for h in range(SHARED)]

                def step(j, state):
                    state = [list(s) for s in state]
                    for u in range(UNROLL):
                        at = pl.multiple_of((j * UNROLL + u) * SPAN, SPAN)
                        for ref, lane in sources:
                            for h in range(SHARED):
                                weight = weights(qs[h], ref, at, lane, SPAN)
                                state[h][0] = state[h][0] + mix(weight, ref, at, lane + HD, SPAN)
                                state[h][1] = state[h][1] + by_lane(weight)
                    return tuple(tuple(s) for s in state)

                zero = jnp.zeros((TILE, HD), jnp.float32)
                state = lax.fori_loop(0, index * (TILE // (SPAN * UNROLL)), step, ((zero, zero),) * SHARED)
                for at in range(0, TILE, PART):
                    row = lax.broadcasted_iota(jnp.int32, (PART, 1), 0) + at
                    token = (row // rows) * (rows * CORES) + core * rows + lax.rem(row, rows)
                    live = first * CORES + token < valid
                    limits = (row, (row // rows + core) * rows - 1)
                    size = at + PART
                    key = lax.broadcasted_iota(jnp.int32, (PART, size), 1)
                    for h in range(SHARED):
                        acc = state[h][0][at:size]
                        total = state[h][1][at:size]
                        for (ref, lane), limit in zip(sources, limits):
                            weight = weights(qs[h][at:size], ref, first, lane, size)
                            weight = jnp.where(key <= limit, weight, 0.0)
                            acc = acc + mix(weight, ref, first, lane + HD, size)
                            total = total + by_lane(weight)
                        result = acc / jnp.sum(total, axis=1, keepdims=True)
                        result = jnp.where(live, result, 0.0).astype(jnp.bfloat16)
                        out[pl.ds(pl.multiple_of(first + at, PART), PART), h * HD : (h + 1) * HD] = result

            @pl.when(first * CORES >= valid)
            def _():
                out[pl.ds(first, TILE), :] = jnp.zeros((TILE, WIDE), jnp.bfloat16)

            return carry

        lax.fori_loop(0, tiles, one_tile, 0)

    return pl.pallas_call(
        body,
        out_shape=jax.ShapeDtypeStruct((length, WIDE), mine.dtype),
        in_specs=[smem(), vmem(), vmem()],
        out_specs=vmem(),
        compiler_params=pltpu.CompilerParams(vmem_limit_bytes=ROOM),
        name="attend",
    )(place, mine, other)


def per_device(queries, keys, values, lengths):
    seqs, rows, _ = queries.shape
    core = lax.axis_index(CORE)
    own_seq = lax.axis_index(RING) // KVH
    valid = jnp.sum(jnp.where(jnp.arange(seqs) == own_seq, lengths, 0))
    place = jnp.stack([core, valid]).astype(jnp.int32)
    blocks = pack(queries, keys, values)
    mine = lax.all_to_all(blocks, RING, 0, 0, tiled=True)
    other = lax.ppermute(mine[:, WIDE:], CORE, [(i, CORES - 1 - i) for i in range(CORES)])
    output = attend(mine, other, place, rows)
    back = lax.all_to_all(output, RING, 0, 0, tiled=True)
    return unpack(back, seqs, rows)


def solution(mesh):
    groups = mesh.shape["groups"]
    torus = Mesh(mesh.devices.reshape(groups, -1, CORES), ("groups", RING, CORE))
    placed = P("groups", (RING, CORE), None)
    return jax.shard_map(
        per_device, mesh=torus, in_specs=(placed, placed, placed, P("groups")), out_specs=placed, check_vma=False
    )
```
